32 devices in a mesh: grp: 4 (over y, x), dev: 8 (over z, core).
Axes of the slice: x: 2, y: 2, z: 4, core: 2. Of those that a mesh axis runs over, the one named last changes fastest.
Arguments:
- table: float32 [262144, 128], P(('grp', 'dev')), may hold values from -6 to 6
- cold_grads: float32 [131072, 128], P(('grp', 'dev')), may hold values from -6 to 6
- cold_owner: int32 [131072, 1], P(('grp', 'dev')), may hold values from 0 to 31; in each aligned block of 4096 rows (0 to 4095, 4096 to 8191, ...) at most 256 rows name the same one
- cold_row: int32 [131072], P(('grp', 'dev')), may hold values from 0 to 8191
- hot_grads: float32 [32768, 128], P(('grp', 'dev')), may hold values from -6 to 6
- hot_slot: int32 [32768], P(('grp', 'dev')), may hold values from 0 to 255
- hot_ids: int32 [256], replicated, may hold values from 0 to 262143, as said below
Outputs:
- new_table: float32 [262144, 128], P(('grp', 'dev'))
The draws below stay inside these ranges and needn't reach their ends.
Inputs may be any that keep to these rules, and one draw needn't show every extreme that they name: `cold_owner`: among the 4096 rare-row lookups of one device no owner is named more than 256 times, a bound that some block reaches. `hot_ids`: all entries differ.
All inputs are finite; a program needn't handle non-finite values.
Results may differ from the reference program's by a relative error of at most 0.00005.
Values sent between devices are 32-bit elements; how exact they have to be, the bound alone decides.
A program may use at most 64 MiB of HBM per device.

```python
import math
import jax
import jax.numpy as jnp
import numpy as np

W = 128
ROWS_DEV = 8192
HOT = 256
COLD_DEV = 4096
CAP = 256
ROWS = 262144
COLD = 131072
HOT_LOOK = 32768
DEVICES = 32


def draw_hot_ids(key, part):
    return jax.random.choice(jax.random.fold_in(key, 7), ROWS, (HOT,), replace=False).astype(jnp.int32)


def plant(array, own_key, smallest, largest):
    index_at = [jax.random.randint(jax.random.fold_in(own_key, axis), (), 0, length) for axis, length in enumerate(array.shape)]
    longest = array.shape.index(max(array.shape))
    next_to = index_at[:longest] + [(index_at[longest] + 1) % array.shape[longest]] + index_at[longest + 1:]
    return array.at[tuple(index_at)].set(smallest).at[tuple(next_to)].set(largest)


def block_scale(own_key, shape, shards, low, high):
    level = 1.0
    for axis_at, blocks in shards:
        heights = jax.random.uniform(jax.random.fold_in(jax.random.fold_in(own_key, 6), axis_at), (blocks,), jnp.float32, low / len(shards), high / len(shards))
        level = level * jnp.repeat(jnp.exp(heights), shape[axis_at] // blocks).reshape((-1,) + (1,) * (len(shape) - 1 - axis_at))
    return level


def deal_out(stream_key, own, number, rows, count, top, most, lean):
    order = jax.random.permutation(stream_key, count)
    packed, common = shares(count, rows * top, most, lean, True), shares(count, rows * top, most, lean, False)
    places = jnp.arange(count)

    def named(sizes, rotation):
        used = int((sizes > 0).sum())
        fixed = max(1, used // 4)
        moved = fixed + (places - fixed + rotation * (used - fixed)) % max(1, count - fixed)
        return jnp.zeros((count,), jnp.int32).at[order[jnp.where(places < fixed, places, moved)]].set(jnp.asarray(sizes, jnp.int32))

    sizes = jnp.where(number % 4 == 0, named(packed, number // 4), named(common, number - number // 4 - 1))
    mixed = jax.random.permutation(jax.random.fold_in(own, 3), count)
    donor, sink = mixed[0:count // 2 * 2:2], mixed[1:count // 2 * 2:2]
    room = jnp.minimum(sizes[donor] - 1, most - sizes[sink]) // 2
    room = jnp.where((donor == order[0]) | (sink == order[0]) | (sizes[sink] == 0), 0, jnp.maximum(room, 0))
    moved = jax.random.randint(jax.random.fold_in(own, 4), (count // 2,), 0, 1 << 20) % (room + 1)
    sizes = sizes.at[donor].add(-moved).at[sink].add(moved)
    members = jnp.searchsorted(jnp.cumsum(sizes), jnp.arange(rows * top), side="right").astype(jnp.int32)
    grid = members.reshape(top, rows).T
    grid = grid[jax.random.permutation(jax.random.fold_in(own, 1), rows)]
    rotation = jax.random.randint(jax.random.fold_in(own, 2), (rows, 1), 0, top)
    return jnp.take_along_axis(grid, (jnp.arange(top)[None, :] + rotation) % top, axis=1)


def shares(count, total, reach, lean, full):
    loads = [(1 << 20) // math.isqrt(grade ** lean) + 1 for grade in range(1, count + 1)]
    largest = reach if full else min(reach, max(-(-total // count), total * loads[0] // sum(loads)))
    least = 1 if total - largest >= count - 1 else 0
    holding, surplus = [largest] + [least] * (count - 1), total - largest - least * (count - 1)
    while surplus > 0:
        free = [i for i in range(1, count) if holding[i] < largest] or [i for i in range(1, count) if holding[i] < reach]
        pool, left = sum([loads[i] for i in free]), surplus
        for i in free:
            addition = min(reach - holding[i], max(1, left * loads[i] // pool), surplus)
            holding[i] = holding[i] + addition
            surplus = surplus - addition
    return np.array(holding)


def gaussian(stream_key, extent, scale, bound, split=(), kind=jnp.bfloat16):
    values = scale * jax.random.normal(stream_key, extent, jnp.float32)
    if split:
        values = values * block_scale(stream_key, extent, split, -0.22, 0.18)
    return jnp.clip(values, -bound, bound).astype(kind)


def setup_inputs(seed: int = 0) -> dict:
    key_list = jax.random.split(jax.random.key(seed), 8)
    table = gaussian(key_list[0], (ROWS, W), 1.0, 6.0, ((0, 32),), jnp.float32)
    cold_grads = gaussian(key_list[1], (COLD, W), 1.0, 6.0, ((0, 32),), jnp.float32)
    cold_owner_keys = jax.random.split(jax.random.fold_in(key_list[2], 1), COLD // COLD_DEV)
    cold_owner_turns = jax.random.permutation(jax.random.fold_in(key_list[2], 3), COLD // COLD_DEV)
    cold_owner = jax.vmap(lambda own, number: deal_out(jax.random.fold_in(key_list[2], 2), own, number, COLD_DEV, DEVICES, 1, CAP, 2))(cold_owner_keys, cold_owner_turns).reshape((COLD, 1))
    cold_row = plant(jax.random.randint(key_list[3], (COLD,), 0, ROWS_DEV), jax.random.fold_in(key_list[3], 1), 0, ROWS_DEV - 1).astype(jnp.int32)
    hot_grads = gaussian(key_list[4], (HOT_LOOK, W), 1.0, 6.0, ((0, 32),), jnp.float32)
    hot_slot = plant(jax.random.randint(key_list[5], (HOT_LOOK,), 0, HOT), jax.random.fold_in(key_list[5], 1), 0, HOT - 1).astype(jnp.int32)
    hot_ids = draw_hot_ids(jax.random.fold_in(key_list[7], 71), 0)
    return {"table": table, "cold_grads": cold_grads, "cold_owner": cold_owner, "cold_row": cold_row, "hot_grads": hot_grads, "hot_slot": hot_slot, "hot_ids": hot_ids}


def reference(table, cold_grads, cold_owner, cold_row, hot_grads, hot_slot, hot_ids):
    cold_id = (cold_owner[:, 0] * ROWS_DEV + cold_row).astype(jnp.int32)
    hot_id = hot_ids[hot_slot].astype(jnp.int32)
    new_table = table.at[cold_id].add(-0.05 * cold_grads)
    new_table = new_table.at[hot_id].add(-0.05 * hot_grads)
    return new_table
```

```python
import functools

import jax
import jax.numpy as jnp
from jax import lax
from jax.experimental import pallas as pl
from jax.experimental.pallas import tpu as pltpu
from jax.sharding import PartitionSpec as P

LEARN = 0.05
MESH = pl.DeviceIdType.MESH
LANES = 128
CHUNK = 256
MIB = 1024 * 1024
TILE = 4096
STEP = 16
AHEAD = 8


def parts_of(values):
    high = values.astype(jnp.bfloat16)
    rest = values - high.astype(jnp.float32)
    middle = rest.astype(jnp.bfloat16)
    low = (rest - middle.astype(jnp.float32)).astype(jnp.bfloat16)
    return high, middle, low


def partner(at, step, size):
    if size & (size - 1):
        return lax.rem(at + step, size), lax.rem(at - step + size, size)
    mixed = 0
    bit = 1
    while bit < size:
        mixed = mixed + bit * lax.rem(at // bit + step // bit, 2)
        bit *= 2
    return mixed, mixed


def spread(i, size):
    if size & (size - 1):
        return i
    turned = 0
    bit = 1
    while bit < size:
        turned = turned + (size // (2 * bit)) * lax.rem(i // bit, 2)
        bit *= 2
    return turned


def plan_kernel(slots, owner_hbm, row_hbm, place, meta, owner, row, spots, s_in):
    devices, lines = meta.shape[0], meta.shape[1]
    deep = lines * LANES
    tall = place.shape[0]
    loads = [pltpu.make_async_copy(owner_hbm, owner, s_in.at[0]), pltpu.make_async_copy(row_hbm, row, s_in.at[1])]
    for load in loads:
        load.start()
    for load in loads:
        load.wait()
    before = lax.broadcasted_iota(jnp.int32, (CHUNK, CHUNK), 0)
    after = lax.broadcasted_iota(jnp.int32, (CHUNK, CHUNK), 1)
    tri = (before <= after).astype(jnp.bfloat16)
    owners = lax.broadcasted_iota(jnp.int32, (tall, CHUNK), 0)
    lane = lax.broadcasted_iota(jnp.int32, (tall, CHUNK), 1).astype(jnp.float32)
    slot = lax.broadcasted_iota(jnp.int32, (deep, CHUNK), 0)
    base = jnp.full((tall, 1), -1.0, jnp.float32)
    found = jnp.zeros((4 * tall, deep), jnp.float32)
    per = CHUNK // LANES
    for b in range(owner.shape[0] // per):
        own = jnp.concatenate([owner[b * per + j:b * per + j + 1, :] for j in range(per)], axis=1)
        at = jnp.concatenate([row[b * per + j:b * per + j + 1, :] for j in range(per)], axis=1)
        hit = own == owners
        run = jnp.dot(hit.astype(jnp.bfloat16), tri, preferred_element_type=jnp.float32) + base
        base = run[:, CHUNK - 1:CHUNK]
        spot = jnp.sum(jnp.where(hit, run, 0.0), axis=0, keepdims=True)
        taken = (slot == (spot + 0.5).astype(jnp.int32)).astype(jnp.bfloat16)
        high = (at // LANES + 1).astype(jnp.float32)
        low = lax.rem(at, LANES).astype(jnp.float32)
        fields = jnp.concatenate([
            jnp.where(hit, float(b), 0.0), jnp.where(hit, lane, 0.0),
            jnp.where(hit, high, 0.0), jnp.where(hit, low, 0.0),
        ], axis=0).astype(jnp.bfloat16)
        found = found + lax.dot_general(
            fields, taken, (((1,), (1,)), ((), ())), preferred_element_type=jnp.float32)
    whole = (found + 0.5).astype(jnp.int32)
    place[...] = whole[:tall] * CHUNK + whole[tall:2 * tall]
    rows = (whole[2 * tall:3 * tall] - 1) * LANES + whole[3 * tall:]
    for j in range(lines):
        spots[j] = rows[:, j * LANES:(j + 1) * LANES]

    def lay_meta(p, carry):
        for j in range(lines):
            meta[p, j:j + 1, :] = spots[j, pl.ds(p, 1), :]
        return carry

    lax.fori_loop(0, devices, lay_meta, 0)


def kernel(
    n_grp, n_dev, slots, place, meta, grads, hot_grads, hot_slot, hot_ids, table_hbm, acc,
    gmeta, send, got, halves, part, rbuf, zbuf, total, s_in, s_meta, r_meta, s_big, r_big, s_hot, r_hot,
):
    devices = n_grp * n_dev
    rows_dev, width = acc.shape
    tile = min(TILE, rows_dev)
    lines = meta.shape[1]
    n_lo = 2 if n_dev % 2 == 0 else 1
    n_hi = n_dev // n_lo
    plane = n_grp * n_lo
    my_grp, my_dev = lax.axis_index("grp"), lax.axis_index("dev")
    my_hi, my_lo = my_dev // n_lo, lax.rem(my_dev, n_lo)
    me = my_grp * n_dev + my_dev
    seat = my_grp * n_lo + my_lo
    here = (my_grp, my_dev)
    barrier = pltpu.get_barrier_semaphore()

    load = pltpu.make_async_copy(table_hbm, acc, s_in)
    load.start()

    def at_step(k, side):
        a = n_grp - 1 - k // n_dev
        b = spread(n_dev - 1 - lax.rem(k, n_dev), n_dev)
        g, d = partner(my_grp, a, n_grp)[side], partner(my_dev, b, n_dev)[side]
        return g * n_dev + d, (g, d)

    def remote(src, dst, ssem, rsem, where):
        return pltpu.make_async_remote_copy(
            src_ref=src, dst_ref=dst, send_sem=ssem, recv_sem=rsem,
            device_id=where, device_id_type=MESH,
        )

    def repeat(first, last, fn):
        def body(k, carry):
            fn(k)
            return carry
        lax.fori_loop(first, last, body, 0)

    repeat(0, devices - 1, lambda k: pl.semaphore_signal(
        barrier, inc=1, device_id=at_step(k, 0)[1], device_id_type=MESH))

    def gather(p, out):
        def body(t, carry):
            first = pl.multiple_of(t * STEP, STEP)
            for j in range(STEP):
                out[p, pl.ds(first + j, 1), :] = grads[pl.ds(place[p, first + j], 1), :]
            return carry
        lax.fori_loop(0, slots // STEP, body, 0)

    def pack(k):
        gather(at_step(k, 0)[0], send)

    def launch(k):
        p, where = at_step(k, 0)
        remote(send.at[p], got.at[me], s_big, r_big.at[k], where).start()

    ahead = min(AHEAD, devices - 1)
    repeat(0, ahead // 2, pack)
    pl.semaphore_wait(barrier, devices - 1)
    repeat(0, ahead // 2, launch)

    def send_meta(k):
        p, where = at_step(k, 0)
        remote(meta.at[p], gmeta.at[me], s_meta, r_meta, where).start()

    repeat(0, devices - 1, send_meta)
    gmeta[me] = meta[me]

    def across(buf_from, at_from, buf_to, at_to, sems):
        def one(j):
            g, lo = partner(my_grp, j // n_lo, n_grp)[0], partner(my_lo, lax.rem(j, n_lo), n_lo)[0]
            src = at_from(g * n_lo + lo)
            remote(buf_from.at[src], buf_to.at[at_to], s_hot.at[sems], r_hot.at[sems], (g, my_hi * n_lo + lo)).start()
        repeat(1, plane, one)

    def finish(buf, count, sems):
        if count:
            most = pl.ds(0, count)
            done = remote(buf.at[most], buf.at[most], s_hot.at[sems], r_hot.at[sems], here)
            done.wait_recv()
            done.wait_send()

    hot = plane * part.shape[1]
    pick = lax.broadcasted_iota(jnp.int32, (hot, hot_grads.shape[0]), 0) == hot_slot[...]
    split = jnp.concatenate(parts_of(hot_grads[...]), axis=1)
    three = jnp.dot(pick.astype(jnp.bfloat16), split, preferred_element_type=jnp.float32)
    part[...] = (three[:, :width] + three[:, width:2 * width] + three[:, 2 * width:]).reshape(part.shape)
    repeat(ahead // 2, ahead, pack)
    repeat(ahead // 2, ahead - 1, launch)
    across(part, lambda other: other, rbuf, seat, 0)
    rbuf[seat] = part[seat]
    gather(me, got)
    load.wait()
    finish(rbuf, plane - 1, 0)
    zbuf[my_hi] = jnp.sum(rbuf[...], axis=0)

    def up(j):
        hi = partner(my_hi, j, n_hi)[0]
        remote(zbuf.at[my_hi], zbuf.at[my_hi], s_hot.at[1], r_hot.at[1], (my_grp, hi * n_lo + my_lo)).start()

    metas = remote(meta.at[pl.ds(0, devices - 1)], gmeta.at[pl.ds(0, devices - 1)], s_meta, r_meta, here)

    def add(values, ids):
        count = values.shape[0]
        high = values.astype(jnp.bfloat16)
        halves[0:count, 0:width] = high
        halves[0:count, width:2 * width] = (values - high.astype(jnp.float32)).astype(jnp.bfloat16)
        spot = lax.broadcasted_iota(jnp.int32, (tile, count), 0)

        def body(t, carry):
            at = pl.multiple_of(t * tile, tile)
            hit = jnp.where(spot == ids - at, 1.0, 0.0).astype(jnp.bfloat16)
            both = jnp.dot(hit, halves[0:count, :], preferred_element_type=jnp.float32)
            w = pl.ds(at, tile)
            acc[w, :] = acc[w, :] - LEARN * (both[:, :width] + both[:, width:])
            return carry

        lax.fori_loop(0, rows_dev // tile, body, 0)

    def turn(i):
        k = lax.rem(i + devices - 1, devices)

        @pl.when(i + ahead < devices - 1)
        def _():
            pack(i + ahead)

        @pl.when(i + ahead < devices)
        def _():
            launch(i + ahead - 1)

        @pl.when(i == 0)
        def _():
            repeat(1, n_hi, up)

        @pl.when(i == 1)
        def _():
            metas.wait_send()
            metas.wait_recv()

        @pl.when(i == devices // 4)
        def _():
            finish(zbuf, n_hi - 1, 1)
            total[seat] = jnp.sum(zbuf[...], axis=0)

        @pl.when(i == devices // 4 + 1)
        def _():
            across(total, lambda other: seat, total, seat, 2)

        @pl.when(i == devices * 5 // 8)
        def _():
            finish(total, plane - 1, 2)
            count = hot_ids.shape[1]
            add(total[...].reshape(-1, width)[:count], hot_ids[...] - me * rows_dev)

        source = at_step(k, 1)[0]

        @pl.when(i > 0)
        def _():
            remote(send.at[0], got.at[source], s_big, r_big.at[k], here).wait_recv()

        info = gmeta[source]
        ids = jnp.concatenate([info[j:j + 1, :] for j in range(lines)], axis=1)[:, :slots]
        add(got[source], ids)

    repeat(0, devices, turn)
    most = pl.ds(0, devices - 1)
    remote(send.at[most], got.at[most], s_big, r_big.at[0], here).wait_send()


def on_device(n_grp, n_dev, table, cold_grads, cold_owner, cold_row, hot_grads, hot_slot, hot_ids):
    devices = n_grp * n_dev
    rows_dev, width = table.shape
    lookups = cold_grads.shape[0]
    looks = hot_grads.shape[0]
    hot = hot_ids.shape[0]
    slots = -(-2 * lookups // devices // STEP) * STEP
    tall = -(-devices // 8) * 8
    lines = -(-slots // LANES)
    n_lo = 2 if n_dev % 2 == 0 else 1
    plane = n_grp * n_lo
    share = -(-hot // (plane * 8)) * 8
    vmem, hbm = pl.BlockSpec(memory_space=pltpu.VMEM), pl.BlockSpec(memory_space=pltpu.HBM)
    f32, i32 = jnp.float32, jnp.int32
    dma = pltpu.SemaphoreType.DMA
    smem = pl.BlockSpec(memory_space=pltpu.SMEM)
    place, meta = pl.pallas_call(
        functools.partial(plan_kernel, slots),
        out_shape=(
            jax.ShapeDtypeStruct((tall, lines * LANES), i32),
            jax.ShapeDtypeStruct((devices, lines, LANES), i32),
        ),
        in_specs=[hbm] * 2,
        out_specs=(vmem,) * 2,
        scratch_shapes=[
            pltpu.VMEM((lookups // LANES, LANES), i32),
            pltpu.VMEM((lookups // LANES, LANES), i32),
            pltpu.VMEM((lines, tall, LANES), i32),
            dma((2,)),
        ],
        compiler_params=pltpu.CompilerParams(vmem_limit_bytes=8 * MIB),
        cost_estimate=pl.CostEstimate(flops=10 ** 9, bytes_accessed=MIB, transcendentals=0),
        name="plan",
    )(cold_owner.reshape(-1, LANES), cold_row.reshape(-1, LANES))
    blocks = (devices, slots, width)
    shares = (plane, share, width)
    return pl.pallas_call(
        functools.partial(kernel, n_grp, n_dev, slots),
        out_shape=jax.ShapeDtypeStruct(table.shape, f32),
        in_specs=[smem, vmem, vmem, vmem, vmem, vmem, hbm],
        out_specs=vmem,
        scratch_shapes=[
            pltpu.VMEM((devices, lines, LANES), i32),
            pltpu.VMEM(blocks, f32),
            pltpu.VMEM(blocks, f32),
            pltpu.VMEM((max(slots, hot), 2 * width), jnp.bfloat16),
            pltpu.VMEM(shares, f32),
            pltpu.VMEM(shares, f32),
            pltpu.VMEM((n_dev // n_lo, share, width), f32),
            pltpu.VMEM(shares, f32),
            dma, dma, dma, dma, dma((devices,)), dma((3,)), dma((3,)),
        ],
        compiler_params=pltpu.CompilerParams(
            collective_id=0, has_side_effects=True, vmem_limit_bytes=44 * MIB
        ),
        name="update",
    )(place, meta, cold_grads, hot_grads, hot_slot.reshape(1, -1), hot_ids.reshape(1, -1), table)


def solution(mesh):
    in_specs = (
        P(("grp", "dev"), None),
        P(("grp", "dev"), None),
        P(("grp", "dev"), None),
        P(("grp", "dev")),
        P(("grp", "dev"), None),
        P(("grp", "dev")),
        P(),
    )
    out_specs = P(("grp", "dev"), None)
    return jax.shard_map(
        functools.partial(on_device, mesh.shape["grp"], mesh.shape["dev"]),
        mesh=mesh, in_specs=in_specs, out_specs=out_specs, check_vma=False,
    )
```

```python
import functools

import jax
import jax.numpy as jnp
from jax import lax
from jax.experimental import pallas as pl
from jax.experimental.pallas import tpu as pltpu
from jax.sharding import PartitionSpec as P

LEARN = 0.05
MESH = pl.DeviceIdType.MESH
LANES = 128
CHUNK = 256
MIB = 1024 * 1024
TILE = 4096
STEP = 16
FINISH = 2048
FIRST, SECOND, THIRD, LAST = 4, 8, 14, 24


def parts_of(values):
    high = values.astype(jnp.bfloat16)
    rest = values - high.astype(jnp.float32)
    middle = rest.astype(jnp.bfloat16)
    low = (rest - middle.astype(jnp.float32)).astype(jnp.bfloat16)
    return high, middle, low


def ids_of(info, slots):
    return jnp.concatenate([info[j:j + 1, :] for j in range(info.shape[0])], axis=1)[:, :slots]


def split_into(halves, values):
    count, width = values.shape
    high = values.astype(jnp.bfloat16)
    halves[0:count, 0:width] = high
    halves[0:count, width:2 * width] = (values - high.astype(jnp.float32)).astype(jnp.bfloat16)


def partner(at, step, size):
    if size & (size - 1):
        return lax.rem(at + step, size), lax.rem(at - step + size, size)
    mixed = 0
    bit = 1
    while bit < size:
        mixed = mixed + bit * lax.rem(at // bit + step // bit, 2)
        bit *= 2
    return mixed, mixed


def spread(i, size):
    if size & (size - 1):
        return i
    turned = 0
    bit = 1
    while bit < size:
        turned = turned + (size // (2 * bit)) * lax.rem(i // bit, 2)
        bit *= 2
    return turned


def plan_kernel(slots, rows_dev, code_ref, place, meta, spots):
    devices, lines = meta.shape[0], meta.shape[1]
    deep = lines * LANES
    tall = place.shape[0]
    before = lax.broadcasted_iota(jnp.int32, (CHUNK, CHUNK), 0)
    after = lax.broadcasted_iota(jnp.int32, (CHUNK, CHUNK), 1)
    tri = (before <= after).astype(jnp.bfloat16)
    owners = lax.broadcasted_iota(jnp.int32, (tall, CHUNK), 0)
    lane = lax.broadcasted_iota(jnp.int32, (tall, CHUNK), 1).astype(jnp.float32)
    slot = lax.broadcasted_iota(jnp.int32, (deep, CHUNK), 0)
    base = jnp.full((tall, 1), -1.0, jnp.float32)
    found = jnp.zeros((4 * tall, deep), jnp.float32)
    per = CHUNK // LANES
    for b in range(code_ref.shape[0] // per):
        code = jnp.concatenate([code_ref[b * per + j:b * per + j + 1, :] for j in range(per)], axis=1)
        own, at = code // rows_dev, lax.rem(code, rows_dev)
        hit = own == owners
        run = jnp.dot(hit.astype(jnp.bfloat16), tri, preferred_element_type=jnp.float32) + base
        base = run[:, CHUNK - 1:CHUNK]
        spot = jnp.sum(jnp.where(hit, run, 0.0), axis=0, keepdims=True)
        taken = (slot == (spot + 0.5).astype(jnp.int32)).astype(jnp.bfloat16)
        high = (at // LANES + 1).astype(jnp.float32)
        low = lax.rem(at, LANES).astype(jnp.float32)
        fields = jnp.concatenate([
            jnp.where(hit, float(b), 0.0), jnp.where(hit, lane, 0.0),
            jnp.where(hit, high, 0.0), jnp.where(hit, low, 0.0),
        ], axis=0).astype(jnp.bfloat16)
        found = found + lax.dot_general(
            fields, taken, (((1,), (1,)), ((), ())), preferred_element_type=jnp.float32)
    whole = (found + 0.5).astype(jnp.int32)
    place[...] = whole[:tall] * CHUNK + whole[tall:2 * tall]
    rows = (whole[2 * tall:3 * tall] - 1) * LANES + whole[3 * tall:]
    for j in range(lines):
        spots[j] = rows[:, j * LANES:(j + 1) * LANES]

    def lay_meta(p, carry):
        for j in range(lines):
            meta[p, j:j + 1, :] = spots[j, pl.ds(p, 1), :]
        return carry

    lax.fori_loop(0, devices, lay_meta, 0)


def kernel(
    n_grp, n_dev, slots, place, meta, grads, hot_grads, hot_slot, hot_ids, table_hbm, acc, block, info,
    gmeta, send, got, halves, part, rbuf, zbuf, total, s_in, s_meta, r_meta, s_big, r_big, s_hot, r_hot,
):
    devices = n_grp * n_dev
    rows_dev, width = acc.shape
    tile = min(TILE, rows_dev)
    lines = meta.shape[1]
    n_lo = 2 if n_dev % 2 == 0 else 1
    n_hi = n_dev // n_lo
    plane = n_grp * n_lo
    my_grp, my_dev = lax.axis_index("grp"), lax.axis_index("dev")
    my_hi, my_lo = my_dev // n_lo, lax.rem(my_dev, n_lo)
    me = my_grp * n_dev + my_dev
    seat = my_grp * n_lo + my_lo
    here = (my_grp, my_dev)
    barrier = pltpu.get_barrier_semaphore()

    load = pltpu.make_async_copy(table_hbm, acc, s_in)
    load.start()

    half = n_dev // 2
    own = half * n_grp

    def at_step(k, side):
        a = lax.rem(k, n_grp)
        b = k // n_grp
        b = jnp.where(a == 0, lax.rem(b + n_dev - half, n_dev), b)
        g, d = partner(my_grp, a, n_grp)[side], partner(my_dev, b, n_dev)[side]
        return g * n_dev + d, (g, d)

    def remote(src, dst, ssem, rsem, where):
        return pltpu.make_async_remote_copy(
            src_ref=src, dst_ref=dst, send_sem=ssem, recv_sem=rsem,
            device_id=where, device_id_type=MESH,
        )

    def repeat(first, last, fn):
        def body(k, carry):
            fn(k)
            return carry
        lax.fori_loop(first, last, body, 0)

    def others(first, last, fn):
        def one(k):
            @pl.when(k != own)
            def _():
                fn(k)
        repeat(first, last, one)

    others(0, devices, lambda k: pl.semaphore_signal(
        barrier, inc=1, device_id=at_step(k, 0)[1], device_id_type=MESH))

    def gather(p, out):
        def body(t, carry):
            first = pl.multiple_of(t * STEP, STEP)
            for j in range(STEP):
                out[p, pl.ds(first + j, 1), :] = grads[pl.ds(place[p, first + j], 1), :]
            return carry
        lax.fori_loop(0, slots // STEP, body, 0)

    def pack(k):
        gather(at_step(k, 0)[0], send)

    def launch(k):
        p, where = at_step(k, 0)
        remote(send.at[p], got.at[me], s_big, r_big.at[k], where).start()

    def pack_then_launch(k):
        pack(k)

        @pl.when(k - 1 != own)
        def _():
            launch(k - 1)

    def send_meta(k):
        p, where = at_step(k, 0)
        remote(meta.at[p], gmeta.at[me], s_meta, r_meta, where).start()

    def across(buf_from, at_from, buf_to, at_to, sems):
        def one(j):
            g, lo = partner(my_grp, j // n_lo, n_grp)[0], partner(my_lo, lax.rem(j, n_lo), n_lo)[0]
            src = at_from(g * n_lo + lo)
            remote(buf_from.at[src], buf_to.at[at_to], s_hot.at[sems], r_hot.at[sems], (g, my_hi * n_lo + lo)).start()
        repeat(1, plane, one)

    def finish(buf, count, sems):
        if count:
            most = pl.ds(0, count)
            done = remote(buf.at[most], buf.at[most], s_hot.at[sems], r_hot.at[sems], here)
            done.wait_recv()
            done.wait_send()

    def up(j):
        hi = partner(my_hi, j, n_hi)[0]
        remote(zbuf.at[my_hi], zbuf.at[my_hi], s_hot.at[1], r_hot.at[1], (my_grp, hi * n_lo + my_lo)).start()

    pack(0)
    pack(1)
    pl.semaphore_wait(barrier, devices - 1)
    launch(0)
    repeat(2, FIRST, pack_then_launch)
    others(0, devices, send_meta)
    hot = plane * part.shape[1]
    pick = lax.broadcasted_iota(jnp.int32, (hot, hot_grads.shape[0]), 0) == hot_slot[...]
    split = jnp.concatenate(parts_of(hot_grads[...]), axis=1)
    three = jnp.dot(pick.astype(jnp.bfloat16), split, preferred_element_type=jnp.float32)
    part[...] = (three[:, :width] + three[:, width:2 * width] + three[:, 2 * width:]).reshape(part.shape)
    gmeta[me] = meta[me]
    rbuf[seat] = part[seat]
    cuts = [FIRST, FIRST + 1, SECOND, SECOND + 1, THIRD, THIRD + 1, devices]
    repeat(cuts[0], cuts[1], pack_then_launch)
    across(part, lambda other: other, rbuf, seat, 0)
    repeat(cuts[1], cuts[2], pack_then_launch)
    finish(rbuf, plane - 1, 0)
    zbuf[my_hi] = jnp.sum(rbuf[...], axis=0)
    repeat(cuts[2], cuts[3], pack_then_launch)
    repeat(1, n_hi, up)
    repeat(cuts[3], cuts[4], pack_then_launch)
    finish(zbuf, n_hi - 1, 1)
    total[seat] = jnp.sum(zbuf[...], axis=0)
    repeat(cuts[4], cuts[5], pack_then_launch)
    across(total, lambda other: seat, total, seat, 2)
    repeat(cuts[5], cuts[6], pack_then_launch)
    gather(me, got)
    others(devices - 1, devices, launch)
    load.wait()

    metas = remote(meta.at[pl.ds(0, devices - 1)], gmeta.at[pl.ds(0, devices - 1)], s_meta, r_meta, here)

    def add(values, ids):
        count = values.shape[0]
        split_into(halves, values)
        spot = lax.broadcasted_iota(jnp.int32, (tile, count), 0)

        def body(t, carry):
            at = pl.multiple_of(t * tile, tile)
            hit = jnp.where(spot == ids - at, 1.0, 0.0).astype(jnp.bfloat16)
            both = jnp.dot(hit, halves[0:count, :], preferred_element_type=jnp.float32)
            w = pl.ds(at, tile)
            acc[w, :] = acc[w, :] - LEARN * (both[:, :width] + both[:, width:])
            return carry

        lax.fori_loop(0, rows_dev // tile, body, 0)

    metas.wait_send()
    metas.wait_recv()

    def turn(k):
        @pl.when(k == LAST)
        def _():
            finish(total, plane - 1, 2)
            count = hot_ids.shape[1]
            add(total[...].reshape(-1, width)[:count], hot_ids[...] - me * rows_dev)

        source = at_step(k, 1)[0]

        @pl.when(k != own)
        def _():
            remote(send.at[0], got.at[source], s_big, r_big.at[k], here).wait_recv()

        @pl.when(k < devices - 1)
        def _():
            add(got[source], ids_of(gmeta[source], slots))

        @pl.when(k == devices - 1)
        def _():
            block[...] = got[source]
            info[...] = gmeta[source]

    repeat(0, devices, turn)
    most = pl.ds(0, devices - 1)
    remote(send.at[most], got.at[most], s_big, r_big.at[0], here).wait_send()


def finish_kernel(slots, acc, block, info, out, ready, halves, sems):
    rows_dev, width = acc.shape
    tile = min(FINISH, rows_dev)
    ids = ids_of(info[...], slots)
    split_into(halves, block[...])
    spot = lax.broadcasted_iota(jnp.int32, (tile, slots), 0)
    copies = []
    for t in range(rows_dev // tile):
        w = pl.ds(t * tile, tile)
        hit = jnp.where(spot == ids - t * tile, 1.0, 0.0).astype(jnp.bfloat16)
        both = jnp.dot(hit, halves[...], preferred_element_type=jnp.float32)
        ready[w, :] = acc[w, :] - LEARN * (both[:, :width] + both[:, width:])
        copies.append(pltpu.make_async_copy(ready.at[w], out.at[w], sems.at[t]))
        copies[-1].start()
    for copy in copies:
        copy.wait()


def on_device(n_grp, n_dev, table, cold_grads, cold_owner, cold_row, hot_grads, hot_slot, hot_ids):
    devices = n_grp * n_dev
    rows_dev, width = table.shape
    lookups = cold_grads.shape[0]
    looks = hot_grads.shape[0]
    hot = hot_ids.shape[0]
    slots = -(-2 * lookups // devices // STEP) * STEP
    tall = -(-devices // 8) * 8
    lines = -(-slots // LANES)
    n_lo = 2 if n_dev % 2 == 0 else 1
    plane = n_grp * n_lo
    share = -(-hot // (plane * 8)) * 8
    vmem, hbm = pl.BlockSpec(memory_space=pltpu.VMEM), pl.BlockSpec(memory_space=pltpu.HBM)
    f32, i32 = jnp.float32, jnp.int32
    dma = pltpu.SemaphoreType.DMA
    smem = pl.BlockSpec(memory_space=pltpu.SMEM)
    place, meta = pl.pallas_call(
        functools.partial(plan_kernel, slots, rows_dev),
        out_shape=(
            jax.ShapeDtypeStruct((tall, lines * LANES), i32),
            jax.ShapeDtypeStruct((devices, lines, LANES), i32),
        ),
        in_specs=[vmem],
        out_specs=(vmem,) * 2,
        scratch_shapes=[pltpu.VMEM((lines, tall, LANES), i32)],
        compiler_params=pltpu.CompilerParams(vmem_limit_bytes=8 * MIB),
        cost_estimate=pl.CostEstimate(flops=10 ** 11, bytes_accessed=MIB, transcendentals=0),
        name="plan",
    )(cold_owner.reshape(-1, LANES) * rows_dev + cold_row.reshape(-1, LANES))
    blocks = (devices, slots, width)
    shares = (plane, share, width)
    acc, block, info = pl.pallas_call(
        functools.partial(kernel, n_grp, n_dev, slots),
        out_shape=(
            jax.ShapeDtypeStruct(table.shape, f32),
            jax.ShapeDtypeStruct(blocks[1:], f32),
            jax.ShapeDtypeStruct((lines, LANES), i32),
        ),
        in_specs=[smem, vmem, vmem, vmem, vmem, vmem, hbm],
        out_specs=(vmem,) * 3,
        scratch_shapes=[
            pltpu.VMEM((devices, lines, LANES), i32),
            pltpu.VMEM(blocks, f32),
            pltpu.VMEM(blocks, f32),
            pltpu.VMEM((max(slots, hot), 2 * width), jnp.bfloat16),
            pltpu.VMEM(shares, f32),
            pltpu.VMEM(shares, f32),
            pltpu.VMEM((n_dev // n_lo, share, width), f32),
            pltpu.VMEM(shares, f32),
            dma, dma, dma, dma, dma((devices,)), dma((3,)), dma((3,)),
        ],
        compiler_params=pltpu.CompilerParams(
            collective_id=0, has_side_effects=True, vmem_limit_bytes=44 * MIB
        ),
        name="update",
    )(place, meta, cold_grads, hot_grads, hot_slot.reshape(1, -1), hot_ids.reshape(1, -1), table)
    return pl.pallas_call(
        functools.partial(finish_kernel, slots),
        out_shape=jax.ShapeDtypeStruct(table.shape, f32),
        in_specs=[vmem] * 3,
        out_specs=hbm,
        scratch_shapes=[
            pltpu.VMEM(table.shape, f32),
            pltpu.VMEM((slots, 2 * width), jnp.bfloat16),
            dma((-(-rows_dev // FINISH),)),
        ],
        compiler_params=pltpu.CompilerParams(vmem_limit_bytes=24 * MIB),
        name="finish",
    )(acc, block, info)


def solution(mesh):
    in_specs = (
        P(("grp", "dev"), None),
        P(("grp", "dev"), None),
        P(("grp", "dev"), None),
        P(("grp", "dev")),
        P(("grp", "dev"), None),
        P(("grp", "dev")),
        P(),
    )
    out_specs = P(("grp", "dev"), None)
    return jax.shard_map(
        functools.partial(on_device, mesh.shape["grp"], mesh.shape["dev"]),
        mesh=mesh, in_specs=in_specs, out_specs=out_specs, check_vma=False,
    )
```

```python
import functools

import jax
import jax.numpy as jnp
from jax import lax
from jax.experimental import pallas as pl
from jax.experimental.pallas import tpu as pltpu
from jax.sharding import PartitionSpec as P

LEARN = 0.05
MESH = pl.DeviceIdType.MESH
LANES = 128
CHUNK = 256
MIB = 1024 * 1024
TILE = 4096
STEP = 16
FINISH = 2048
FIRST, SECOND, THIRD, LAST = 4, 8, 14, 24


def parts_of(values):
    high = values.astype(jnp.bfloat16)
    rest = values - high.astype(jnp.float32)
    middle = rest.astype(jnp.bfloat16)
    low = (rest - middle.astype(jnp.float32)).astype(jnp.bfloat16)
    return high, middle, low


def ids_of(info, slots):
    return jnp.concatenate([info[j:j + 1, :] for j in range(info.shape[0])], axis=1)[:, :slots]


def split_into(halves, values):
    count, width = values.shape
    high = values.astype(jnp.bfloat16)
    halves[0:count, 0:width] = high
    halves[0:count, width:2 * width] = (values - high.astype(jnp.float32)).astype(jnp.bfloat16)


def partner(at, step, size):
    if size & (size - 1):
        return lax.rem(at + step, size), lax.rem(at - step + size, size)
    mixed = 0
    bit = 1
    while bit < size:
        mixed = mixed + bit * lax.rem(at // bit + step // bit, 2)
        bit *= 2
    return mixed, mixed


def spread(i, size):
    if size & (size - 1):
        return i
    turned = 0
    bit = 1
    while bit < size:
        turned = turned + (size // (2 * bit)) * lax.rem(i // bit, 2)
        bit *= 2
    return turned


def plan_kernel(slots, rows_dev, code_ref, place, meta, spots):
    devices, lines = meta.shape[0], meta.shape[1]
    deep = lines * LANES
    tall = place.shape[0]
    before = lax.broadcasted_iota(jnp.int32, (CHUNK, CHUNK), 0)
    after = lax.broadcasted_iota(jnp.int32, (CHUNK, CHUNK), 1)
    tri = (before <= after).astype(jnp.bfloat16)
    owners = lax.broadcasted_iota(jnp.int32, (tall, CHUNK), 0)
    lane = lax.broadcasted_iota(jnp.int32, (tall, CHUNK), 1).astype(jnp.float32)
    slot = lax.broadcasted_iota(jnp.int32, (deep, CHUNK), 0)
    base = jnp.full((tall, 1), -1.0, jnp.float32)
    found = jnp.zeros((4 * tall, deep), jnp.float32)
    per = CHUNK // LANES
    for b in range(code_ref.shape[0] // per):
        code = jnp.concatenate([code_ref[b * per + j:b * per + j + 1, :] for j in range(per)], axis=1)
        own, at = code // rows_dev, lax.rem(code, rows_dev)
        hit = own == owners
        run = jnp.dot(hit.astype(jnp.bfloat16), tri, preferred_element_type=jnp.float32) + base
        base = run[:, CHUNK - 1:CHUNK]
        spot = jnp.sum(jnp.where(hit, run, 0.0), axis=0, keepdims=True)
        taken = (slot == (spot + 0.5).astype(jnp.int32)).astype(jnp.bfloat16)
        high = (at // LANES + 1).astype(jnp.float32)
        low = lax.rem(at, LANES).astype(jnp.float32)
        fields = jnp.concatenate([
            jnp.where(hit, float(b), 0.0), jnp.where(hit, lane, 0.0),
            jnp.where(hit, high, 0.0), jnp.where(hit, low, 0.0),
        ], axis=0).astype(jnp.bfloat16)
        found = found + lax.dot_general(
            fields, taken, (((1,), (1,)), ((), ())), preferred_element_type=jnp.float32)
    whole = (found + 0.5).astype(jnp.int32)
    place[...] = whole[:tall] * CHUNK + whole[tall:2 * tall]
    rows = (whole[2 * tall:3 * tall] - 1) * LANES + whole[3 * tall:]
    for j in range(lines):
        spots[j] = rows[:, j * LANES:(j + 1) * LANES]

    def lay_meta(p, carry):
        for j in range(lines):
            meta[p, j:j + 1, :] = spots[j, pl.ds(p, 1), :]
        return carry

    lax.fori_loop(0, devices, lay_meta, 0)


def kernel(
    n_grp, n_dev, slots, place, meta, grads, hot_grads, hot_slot, hot_ids, table_hbm, acc, block, info,
    gmeta, send, got, halves, part, rbuf, zbuf, total, s_in, s_meta, r_meta, s_big, r_big, s_hot, r_hot,
):
    devices = n_grp * n_dev
    rows_dev, width = acc.shape
    tile = min(TILE, rows_dev)
    lines = meta.shape[1]
    n_lo = n_dev // 2 if n_dev % 2 == 0 else 1
    n_hi = n_dev // n_lo
    plane = n_grp * n_lo
    my_grp, my_dev = lax.axis_index("grp"), lax.axis_index("dev")
    my_hi, my_lo = my_dev // n_lo, lax.rem(my_dev, n_lo)
    me = my_grp * n_dev + my_dev
    seat = my_grp * n_lo + my_lo
    here = (my_grp, my_dev)
    barrier = pltpu.get_barrier_semaphore()

    load = pltpu.make_async_copy(table_hbm, acc, s_in)
    load.start()

    half = n_dev // 2
    own = half * n_grp

    def at_step(k, side):
        a = lax.rem(k, n_grp)
        b = k // n_grp
        b = jnp.where(a == 0, lax.rem(b + n_dev - half, n_dev), b)
        g, d = partner(my_grp, a, n_grp)[side], partner(my_dev, b, n_dev)[side]
        return g * n_dev + d, (g, d)

    def remote(src, dst, ssem, rsem, where):
        return pltpu.make_async_remote_copy(
            src_ref=src, dst_ref=dst, send_sem=ssem, recv_sem=rsem,
            device_id=where, device_id_type=MESH,
        )

    def repeat(first, last, fn):
        def body(k, carry):
            fn(k)
            return carry
        lax.fori_loop(first, last, body, 0)

    def others(first, last, fn):
        def one(k):
            @pl.when(k != own)
            def _():
                fn(k)
        repeat(first, last, one)

    for g in range(n_grp):
        def greet(d, g=g):
            @pl.when(g * n_dev + d != me)
            def _():
                pl.semaphore_signal(barrier, inc=1, device_id=(g, d), device_id_type=MESH)
        repeat(0, n_dev, greet)

    def gather(p, out):
        def body(t, carry):
            first = pl.multiple_of(t * STEP, STEP)
            for j in range(STEP):
                out[p, pl.ds(first + j, 1), :] = grads[pl.ds(place[p, first + j], 1), :]
            return carry
        lax.fori_loop(0, slots // STEP, body, 0)

    def pack(k):
        gather(at_step(k, 0)[0], send)

    def launch(k):
        p, where = at_step(k, 0)
        remote(send.at[p], got.at[me], s_big, r_big.at[k], where).start()

    def pack_then_launch(k):
        pack(k)

        @pl.when(k - 1 != own)
        def _():
            launch(k - 1)

    def send_meta(k):
        p, where = at_step(k, 0)
        remote(meta.at[p], gmeta.at[me], s_meta, r_meta, where).start()

    def across(buf_from, at_from, buf_to, at_to, sems):
        def one(j):
            g, lo = partner(my_grp, j // n_lo, n_grp)[0], partner(my_lo, lax.rem(j, n_lo), n_lo)[0]
            src = at_from(g * n_lo + lo)
            remote(buf_from.at[src], buf_to.at[at_to], s_hot.at[sems], r_hot.at[sems], (g, my_hi * n_lo + lo)).start()
        repeat(1, plane, one)

    def finish(buf, count, sems):
        if count:
            most = pl.ds(0, count)
            done = remote(buf.at[most], buf.at[most], s_hot.at[sems], r_hot.at[sems], here)
            done.wait_recv()
            done.wait_send()

    def up(j):
        hi = partner(my_hi, j, n_hi)[0]
        remote(zbuf.at[my_hi], zbuf.at[my_hi], s_hot.at[1], r_hot.at[1], (my_grp, hi * n_lo + my_lo)).start()

    pack(0)
    pack(1)
    pl.semaphore_wait(barrier, devices - 1)
    launch(0)
    repeat(2, FIRST, pack_then_launch)
    others(0, devices, send_meta)
    hot = plane * part.shape[1]
    pick = lax.broadcasted_iota(jnp.int32, (hot, hot_grads.shape[0]), 0) == hot_slot[...]
    split = jnp.concatenate(parts_of(hot_grads[...]), axis=1)
    three = jnp.dot(pick.astype(jnp.bfloat16), split, preferred_element_type=jnp.float32)
    part[...] = (three[:, :width] + three[:, width:2 * width] + three[:, 2 * width:]).reshape(part.shape)
    gmeta[me] = meta[me]
    rbuf[seat] = part[seat]
    cuts = [FIRST, FIRST + 1, SECOND, SECOND + 1, THIRD, THIRD + 1, devices]
    repeat(cuts[0], cuts[1], pack_then_launch)
    across(part, lambda other: other, rbuf, seat, 0)
    repeat(cuts[1], cuts[2], pack_then_launch)
    finish(rbuf, plane - 1, 0)
    zbuf[my_hi] = jnp.sum(rbuf[...], axis=0)
    repeat(cuts[2], cuts[3], pack_then_launch)
    repeat(1, n_hi, up)
    repeat(cuts[3], cuts[4], pack_then_launch)
    finish(zbuf, n_hi - 1, 1)
    total[seat] = jnp.sum(zbuf[...], axis=0)
    repeat(cuts[4], cuts[5], pack_then_launch)
    across(total, lambda other: seat, total, seat, 2)
    repeat(cuts[5], cuts[6], pack_then_launch)
    gather(me, got)
    others(devices - 1, devices, launch)
    load.wait()

    metas = remote(meta.at[pl.ds(0, devices - 1)], gmeta.at[pl.ds(0, devices - 1)], s_meta, r_meta, here)

    def add(values, ids):
        count = values.shape[0]
        split_into(halves, values)
        spot = lax.broadcasted_iota(jnp.int32, (tile, count), 0)

        def body(t, carry):
            at = pl.multiple_of(t * tile, tile)
            hit = jnp.where(spot == ids - at, 1.0, 0.0).astype(jnp.bfloat16)
            both = jnp.dot(hit, halves[0:count, :], preferred_element_type=jnp.float32)
            w = pl.ds(at, tile)
            acc[w, :] = acc[w, :] - LEARN * (both[:, :width] + both[:, width:])
            return carry

        lax.fori_loop(0, rows_dev // tile, body, 0)

    metas.wait_send()
    metas.wait_recv()

    def turn(k):
        @pl.when(k == LAST)
        def _():
            finish(total, plane - 1, 2)
            count = hot_ids.shape[1]
            add(total[...].reshape(-1, width)[:count], hot_ids[...] - me * rows_dev)

        source = at_step(k, 1)[0]

        @pl.when(k != own)
        def _():
            remote(send.at[0], got.at[source], s_big, r_big.at[k], here).wait_recv()

        @pl.when(k < devices - 1)
        def _():
            add(got[source], ids_of(gmeta[source], slots))

        @pl.when(k == devices - 1)
        def _():
            block[...] = got[source]
            info[...] = gmeta[source]

    repeat(0, devices, turn)
    most = pl.ds(0, devices - 1)
    remote(send.at[most], got.at[most], s_big, r_big.at[0], here).wait_send()


def finish_kernel(slots, acc, block, info, out, ready, halves, sems):
    rows_dev, width = acc.shape
    tile = min(FINISH, rows_dev)
    ids = ids_of(info[...], slots)
    split_into(halves, block[...])
    spot = lax.broadcasted_iota(jnp.int32, (tile, slots), 0)
    copies = []
    for t in range(rows_dev // tile):
        w = pl.ds(t * tile, tile)
        hit = jnp.where(spot == ids - t * tile, 1.0, 0.0).astype(jnp.bfloat16)
        both = jnp.dot(hit, halves[...], preferred_element_type=jnp.float32)
        ready[w, :] = acc[w, :] - LEARN * (both[:, :width] + both[:, width:])
        copies.append(pltpu.make_async_copy(ready.at[w], out.at[w], sems.at[t]))
        copies[-1].start()
    for copy in copies:
        copy.wait()


def on_device(n_grp, n_dev, table, cold_grads, cold_owner, cold_row, hot_grads, hot_slot, hot_ids):
    devices = n_grp * n_dev
    rows_dev, width = table.shape
    lookups = cold_grads.shape[0]
    looks = hot_grads.shape[0]
    hot = hot_ids.shape[0]
    slots = -(-2 * lookups // devices // STEP) * STEP
    tall = -(-devices // 8) * 8
    lines = -(-slots // LANES)
    n_lo = n_dev // 2 if n_dev % 2 == 0 else 1
    plane = n_grp * n_lo
    share = -(-hot // (plane * 8)) * 8
    vmem, hbm = pl.BlockSpec(memory_space=pltpu.VMEM), pl.BlockSpec(memory_space=pltpu.HBM)
    f32, i32 = jnp.float32, jnp.int32
    dma = pltpu.SemaphoreType.DMA
    smem = pl.BlockSpec(memory_space=pltpu.SMEM)
    place, meta = pl.pallas_call(
        functools.partial(plan_kernel, slots, rows_dev),
        out_shape=(
            jax.ShapeDtypeStruct((tall, lines * LANES), i32),
            jax.ShapeDtypeStruct((devices, lines, LANES), i32),
        ),
        in_specs=[vmem],
        out_specs=(vmem,) * 2,
        scratch_shapes=[pltpu.VMEM((lines, tall, LANES), i32)],
        compiler_params=pltpu.CompilerParams(vmem_limit_bytes=8 * MIB),
        cost_estimate=pl.CostEstimate(flops=10 ** 11, bytes_accessed=MIB, transcendentals=0),
        name="plan",
    )((cold_owner * rows_dev + cold_row.reshape(-1, 1)).reshape(-1, LANES))
    blocks = (devices, slots, width)
    shares = (plane, share, width)
    acc, block, info = pl.pallas_call(
        functools.partial(kernel, n_grp, n_dev, slots),
        out_shape=(
            jax.ShapeDtypeStruct(table.shape, f32),
            jax.ShapeDtypeStruct(blocks[1:], f32),
            jax.ShapeDtypeStruct((lines, LANES), i32),
        ),
        in_specs=[smem, vmem, vmem, vmem, vmem, vmem, hbm],
        out_specs=(vmem,) * 3,
        scratch_shapes=[
            pltpu.VMEM((devices, lines, LANES), i32),
            pltpu.VMEM(blocks, f32),
            pltpu.VMEM(blocks, f32),
            pltpu.VMEM((max(slots, hot), 2 * width), jnp.bfloat16),
            pltpu.VMEM(shares, f32),
            pltpu.VMEM(shares, f32),
            pltpu.VMEM((n_dev // n_lo, share, width), f32),
            pltpu.VMEM(shares, f32),
            dma, dma, dma, dma, dma((devices,)), dma((3,)), dma((3,)),
        ],
        compiler_params=pltpu.CompilerParams(
            collective_id=0, has_side_effects=True, vmem_limit_bytes=44 * MIB
        ),
        name="update",
    )(place, meta, cold_grads, hot_grads, hot_slot.reshape(1, -1), hot_ids.reshape(1, -1), table)
    return pl.pallas_call(
        functools.partial(finish_kernel, slots),
        out_shape=jax.ShapeDtypeStruct(table.shape, f32),
        in_specs=[vmem] * 3,
        out_specs=hbm,
        scratch_shapes=[
            pltpu.VMEM(table.shape, f32),
            pltpu.VMEM((slots, 2 * width), jnp.bfloat16),
            dma((-(-rows_dev // FINISH),)),
        ],
        compiler_params=pltpu.CompilerParams(vmem_limit_bytes=24 * MIB),
        name="finish",
    )(acc, block, info)


def solution(mesh):
    in_specs = (
        P(("grp", "dev"), None),
        P(("grp", "dev"), None),
        P(("grp", "dev"), None),
        P(("grp", "dev")),
        P(("grp", "dev"), None),
        P(("grp", "dev")),
        P(),
    )
    out_specs = P(("grp", "dev"), None)
    return jax.shard_map(
        functools.partial(on_device, mesh.shape["grp"], mesh.shape["dev"]),
        mesh=mesh, in_specs=in_specs, out_specs=out_specs, check_vma=False,
    )
```

```python
import functools

import jax
import jax.numpy as jnp
from jax import lax
from jax.experimental import pallas as pl
from jax.experimental.pallas import tpu as pltpu
from jax.sharding import PartitionSpec as P

LEARN = 0.05
MESH = pl.DeviceIdType.MESH
LANES = 128
CHUNK = 256
MIB = 1024 * 1024
TILE = 4096
STEP = 16
FINISH = 1024
FIRST, SECOND, THIRD, LAST = 4, 8, 14, 24


def parts_of(values):
    high = values.astype(jnp.bfloat16)
    rest = values - high.astype(jnp.float32)
    middle = rest.astype(jnp.bfloat16)
    low = (rest - middle.astype(jnp.float32)).astype(jnp.bfloat16)
    return high, middle, low


def ids_of(info, slots):
    return jnp.concatenate([info[j:j + 1, :] for j in range(info.shape[0])], axis=1)[:, :slots]


def split_into(halves, values):
    count, width = values.shape
    high = values.astype(jnp.bfloat16)
    halves[0:count, 0:width] = high
    halves[0:count, width:2 * width] = (values - high.astype(jnp.float32)).astype(jnp.bfloat16)


def partner(at, step, size):
    if size & (size - 1):
        return lax.rem(at + step, size), lax.rem(at - step + size, size)
    mixed = 0
    bit = 1
    while bit < size:
        mixed = mixed + bit * lax.rem(at // bit + step // bit, 2)
        bit *= 2
    return mixed, mixed


def spread(i, size):
    if size & (size - 1):
        return i
    turned = 0
    bit = 1
    while bit < size:
        turned = turned + (size // (2 * bit)) * lax.rem(i // bit, 2)
        bit *= 2
    return turned


def plan_kernel(slots, rows_dev, code_ref, place, meta, spots):
    devices, lines = meta.shape[0], meta.shape[1]
    deep = lines * LANES
    tall = place.shape[0]
    before = lax.broadcasted_iota(jnp.int32, (CHUNK, CHUNK), 0)
    after = lax.broadcasted_iota(jnp.int32, (CHUNK, CHUNK), 1)
    tri = (before <= after).astype(jnp.bfloat16)
    owners = lax.broadcasted_iota(jnp.int32, (tall, CHUNK), 0)
    lane = lax.broadcasted_iota(jnp.int32, (tall, CHUNK), 1).astype(jnp.float32)
    slot = lax.broadcasted_iota(jnp.int32, (deep, CHUNK), 0)
    base = jnp.full((tall, 1), -1.0, jnp.float32)
    left, right = [], []
    per = CHUNK // LANES
    for b in range(code_ref.shape[0] // per):
        code = jnp.concatenate([code_ref[b * per + j:b * per + j + 1, :] for j in range(per)], axis=1)
        own, at = code // rows_dev, lax.rem(code, rows_dev)
        hit = own == owners
        run = jnp.dot(hit.astype(jnp.bfloat16), tri, preferred_element_type=jnp.float32) + base
        base = run[:, CHUNK - 1:CHUNK]
        spot = jnp.sum(jnp.where(hit, run, 0.0), axis=0, keepdims=True)
        taken = (slot == (spot + 0.5).astype(jnp.int32)).astype(jnp.bfloat16)
        high = (at // LANES + 1).astype(jnp.float32)
        low = lax.rem(at, LANES).astype(jnp.float32)
        fields = jnp.concatenate([
            jnp.where(hit, float(b), 0.0), jnp.where(hit, lane, 0.0),
            jnp.where(hit, high, 0.0), jnp.where(hit, low, 0.0),
        ], axis=0).astype(jnp.bfloat16)
        left.append(fields)
        right.append(taken)
    found = lax.dot_general(
        jnp.concatenate(left, axis=1), jnp.concatenate(right, axis=1),
        (((1,), (1,)), ((), ())), preferred_element_type=jnp.float32)
    whole = (found + 0.5).astype(jnp.int32)
    place[...] = whole[:tall] * CHUNK + whole[tall:2 * tall]
    rows = (whole[2 * tall:3 * tall] - 1) * LANES + whole[3 * tall:]
    for j in range(lines):
        spots[j] = rows[:, j * LANES:(j + 1) * LANES]

    def lay_meta(p, carry):
        for j in range(lines):
            meta[p, j:j + 1, :] = spots[j, pl.ds(p, 1), :]
        return carry

    lax.fori_loop(0, devices, lay_meta, 0, unroll=8 if devices % 8 == 0 else 1)


def kernel(
    n_grp, n_dev, slots, place, meta, grads, hot_grads, hot_slot, hot_ids, table_hbm, acc, block, info,
    gmeta, send, got, halves, part, rbuf, zbuf, total, s_in, s_meta, r_meta, s_big, r_big, s_hot, r_hot,
):
    devices = n_grp * n_dev
    rows_dev, width = acc.shape
    tile = min(TILE, rows_dev)
    lines = meta.shape[1]
    n_lo = n_dev // 2 if n_dev % 2 == 0 else 1
    n_hi = n_dev // n_lo
    plane = n_grp * n_lo
    my_grp, my_dev = lax.axis_index("grp"), lax.axis_index("dev")
    my_hi, my_lo = my_dev // n_lo, lax.rem(my_dev, n_lo)
    me = my_grp * n_dev + my_dev
    seat = my_grp * n_lo + my_lo
    here = (my_grp, my_dev)
    barrier = pltpu.get_barrier_semaphore()

    load = pltpu.make_async_copy(table_hbm, acc, s_in)
    load.start()

    half = n_dev // 2
    own = half * n_grp

    def at_step(k, side):
        a = lax.rem(k, n_grp)
        b = k // n_grp
        b = jnp.where(a == 0, lax.rem(b + n_dev - half, n_dev), b)
        g, d = partner(my_grp, a, n_grp)[side], partner(my_dev, b, n_dev)[side]
        return g * n_dev + d, (g, d)

    def remote(src, dst, ssem, rsem, where):
        return pltpu.make_async_remote_copy(
            src_ref=src, dst_ref=dst, send_sem=ssem, recv_sem=rsem,
            device_id=where, device_id_type=MESH,
        )

    def repeat(first, last, fn):
        def body(k, carry):
            fn(k)
            return carry
        lax.fori_loop(first, last, body, 0)

    def others(first, last, fn):
        def one(k):
            @pl.when(k != own)
            def _():
                fn(k)
        repeat(first, last, one)

    for g in range(n_grp):
        def greet(d, g=g):
            @pl.when(g * n_dev + d != me)
            def _():
                pl.semaphore_signal(barrier, inc=1, device_id=(g, d), device_id_type=MESH)
        repeat(0, n_dev, greet)

    def gather(p, out):
        def body(t, carry):
            first = pl.multiple_of(t * STEP, STEP)
            for j in range(STEP):
                out[p, pl.ds(first + j, 1), :] = grads[pl.ds(place[p, first + j], 1), :]
            return carry
        lax.fori_loop(0, slots // STEP, body, 0)

    def pack(k):
        gather(at_step(k, 0)[0], send)

    def launch(k):
        p, where = at_step(k, 0)
        remote(send.at[p], got.at[me], s_big, r_big.at[k], where).start()

    def pack_then_launch(k):
        pack(k)

        @pl.when(k - 1 != own)
        def _():
            launch(k - 1)

    def send_meta(k):
        p, where = at_step(k, 0)
        remote(meta.at[p], gmeta.at[me], s_meta, r_meta, where).start()

    def across(buf_from, at_from, buf_to, at_to, sems):
        def one(j):
            g, lo = partner(my_grp, j // n_lo, n_grp)[0], partner(my_lo, lax.rem(j, n_lo), n_lo)[0]
            src = at_from(g * n_lo + lo)
            remote(buf_from.at[src], buf_to.at[at_to], s_hot.at[sems], r_hot.at[sems], (g, my_hi * n_lo + lo)).start()
        repeat(1, plane, one)

    def finish(buf, count, sems):
        if count:
            most = pl.ds(0, count)
            done = remote(buf.at[most], buf.at[most], s_hot.at[sems], r_hot.at[sems], here)
            done.wait_recv()
            done.wait_send()

    def up(j):
        hi = partner(my_hi, j, n_hi)[0]
        remote(zbuf.at[my_hi], zbuf.at[my_hi], s_hot.at[1], r_hot.at[1], (my_grp, hi * n_lo + my_lo)).start()

    pack(0)
    pack(1)
    pl.semaphore_wait(barrier, devices - 1)
    launch(0)
    repeat(2, FIRST, pack_then_launch)
    others(0, devices, send_meta)
    hot = plane * part.shape[1]
    pick = lax.broadcasted_iota(jnp.int32, (hot, hot_grads.shape[0]), 0) == hot_slot[...]
    split = jnp.concatenate(parts_of(hot_grads[...]), axis=1)
    three = jnp.dot(pick.astype(jnp.bfloat16), split, preferred_element_type=jnp.float32)
    part[...] = (three[:, :width] + three[:, width:2 * width] + three[:, 2 * width:]).reshape(part.shape)
    gmeta[me] = meta[me]
    rbuf[seat] = part[seat]
    cuts = [FIRST, FIRST + 1, SECOND, SECOND + 1, THIRD, THIRD + 1, devices]
    repeat(cuts[0], cuts[1], pack_then_launch)
    across(part, lambda other: other, rbuf, seat, 0)
    repeat(cuts[1], cuts[2], pack_then_launch)
    finish(rbuf, plane - 1, 0)
    zbuf[my_hi] = jnp.sum(rbuf[...], axis=0)
    repeat(cuts[2], cuts[3], pack_then_launch)
    repeat(1, n_hi, up)
    repeat(cuts[3], cuts[4], pack_then_launch)
    finish(zbuf, n_hi - 1, 1)
    total[seat] = jnp.sum(zbuf[...], axis=0)
    repeat(cuts[4], cuts[5], pack_then_launch)
    across(total, lambda other: seat, total, seat, 2)
    repeat(cuts[5], cuts[6], pack_then_launch)
    gather(me, got)
    others(devices - 1, devices, launch)
    load.wait()

    metas = remote(meta.at[pl.ds(0, devices - 1)], gmeta.at[pl.ds(0, devices - 1)], s_meta, r_meta, here)

    def add(values, ids):
        count = values.shape[0]
        split_into(halves, values)
        spot = lax.broadcasted_iota(jnp.int32, (tile, count), 0)

        def body(t, carry):
            at = pl.multiple_of(t * tile, tile)
            hit = jnp.where(spot == ids - at, 1.0, 0.0).astype(jnp.bfloat16)
            both = jnp.dot(hit, halves[0:count, :], preferred_element_type=jnp.float32)
            w = pl.ds(at, tile)
            acc[w, :] = acc[w, :] - LEARN * (both[:, :width] + both[:, width:])
            return carry

        lax.fori_loop(0, rows_dev // tile, body, 0)

    metas.wait_send()
    metas.wait_recv()

    def turn(k):
        @pl.when(k == LAST)
        def _():
            finish(total, plane - 1, 2)
            count = hot_ids.shape[1]
            add(total[...].reshape(-1, width)[:count], hot_ids[...] - me * rows_dev)

        source = at_step(k, 1)[0]

        @pl.when(k != own)
        def _():
            remote(send.at[0], got.at[source], s_big, r_big.at[k], here).wait_recv()

        @pl.when(k < devices - 1)
        def _():
            add(got[source], ids_of(gmeta[source], slots))

        @pl.when(k == devices - 1)
        def _():
            block[...] = got[source]
            info[...] = gmeta[source]

    repeat(0, devices, turn)
    most = pl.ds(0, devices - 1)
    remote(send.at[most], got.at[most], s_big, r_big.at[0], here).wait_send()


def finish_kernel(slots, acc, block, info, out, ready, halves, sems):
    rows_dev, width = acc.shape
    tile = min(FINISH, rows_dev)
    ids = ids_of(info[...], slots)
    split_into(halves, block[...])
    spot = lax.broadcasted_iota(jnp.int32, (tile, slots), 0)
    copies = []
    for t in range(rows_dev // tile):
        w = pl.ds(t * tile, tile)
        hit = jnp.where(spot == ids - t * tile, 1.0, 0.0).astype(jnp.bfloat16)
        both = jnp.dot(hit, halves[...], preferred_element_type=jnp.float32)
        ready[w, :] = acc[w, :] - LEARN * (both[:, :width] + both[:, width:])
        copies.append(pltpu.make_async_copy(ready.at[w], out.at[w], sems.at[t]))
        copies[-1].start()
    for copy in copies:
        copy.wait()


def on_device(n_grp, n_dev, table, cold_grads, cold_owner, cold_row, hot_grads, hot_slot, hot_ids):
    devices = n_grp * n_dev
    rows_dev, width = table.shape
    lookups = cold_grads.shape[0]
    looks = hot_grads.shape[0]
    hot = hot_ids.shape[0]
    slots = -(-2 * lookups // devices // STEP) * STEP
    tall = -(-devices // 8) * 8
    lines = -(-slots // LANES)
    n_lo = n_dev // 2 if n_dev % 2 == 0 else 1
    plane = n_grp * n_lo
    share = -(-hot // (plane * 8)) * 8
    vmem, hbm = pl.BlockSpec(memory_space=pltpu.VMEM), pl.BlockSpec(memory_space=pltpu.HBM)
    f32, i32 = jnp.float32, jnp.int32
    dma = pltpu.SemaphoreType.DMA
    smem = pl.BlockSpec(memory_space=pltpu.SMEM)
    place, meta = pl.pallas_call(
        functools.partial(plan_kernel, slots, rows_dev),
        out_shape=(
            jax.ShapeDtypeStruct((tall, lines * LANES), i32),
            jax.ShapeDtypeStruct((devices, lines, LANES), i32),
        ),
        in_specs=[vmem],
        out_specs=(vmem,) * 2,
        scratch_shapes=[pltpu.VMEM((lines, tall, LANES), i32)],
        compiler_params=pltpu.CompilerParams(vmem_limit_bytes=8 * MIB),
        cost_estimate=pl.CostEstimate(flops=10 ** 11, bytes_accessed=MIB, transcendentals=0),
        name="plan",
    )((cold_owner * rows_dev + cold_row.reshape(-1, 1)).reshape(-1, LANES))
    blocks = (devices, slots, width)
    shares = (plane, share, width)
    acc, block, info = pl.pallas_call(
        functools.partial(kernel, n_grp, n_dev, slots),
        out_shape=(
            jax.ShapeDtypeStruct(table.shape, f32),
            jax.ShapeDtypeStruct(blocks[1:], f32),
            jax.ShapeDtypeStruct((lines, LANES), i32),
        ),
        in_specs=[smem, vmem, vmem, vmem, vmem, vmem, hbm],
        out_specs=(vmem,) * 3,
        scratch_shapes=[
            pltpu.VMEM((devices, lines, LANES), i32),
            pltpu.VMEM(blocks, f32),
            pltpu.VMEM(blocks, f32),
            pltpu.VMEM((max(slots, hot), 2 * width), jnp.bfloat16),
            pltpu.VMEM(shares, f32),
            pltpu.VMEM(shares, f32),
            pltpu.VMEM((n_dev // n_lo, share, width), f32),
            pltpu.VMEM(shares, f32),
            dma, dma, dma, dma, dma((devices,)), dma((3,)), dma((3,)),
        ],
        compiler_params=pltpu.CompilerParams(
            collective_id=0, has_side_effects=True, vmem_limit_bytes=44 * MIB
        ),
        name="update",
    )(place, meta, cold_grads, hot_grads, hot_slot.reshape(1, -1), hot_ids.reshape(1, -1), table)
    return pl.pallas_call(
        functools.partial(finish_kernel, slots),
        out_shape=jax.ShapeDtypeStruct(table.shape, f32),
        in_specs=[vmem] * 3,
        out_specs=hbm,
        scratch_shapes=[
            pltpu.VMEM(table.shape, f32),
            pltpu.VMEM((slots, 2 * width), jnp.bfloat16),
            dma((-(-rows_dev // FINISH),)),
        ],
        compiler_params=pltpu.CompilerParams(vmem_limit_bytes=24 * MIB),
        name="finish",
    )(acc, block, info)


def solution(mesh):
    in_specs = (
        P(("grp", "dev"), None),
        P(("grp", "dev"), None),
        P(("grp", "dev"), None),
        P(("grp", "dev")),
        P(("grp", "dev"), None),
        P(("grp", "dev")),
        P(),
    )
    out_specs = P(("grp", "dev"), None)
    return jax.shard_map(
        functools.partial(on_device, mesh.shape["grp"], mesh.shape["dev"]),
        mesh=mesh, in_specs=in_specs, out_specs=out_specs, check_vma=False,
    )
```

```python
import functools

import jax
import jax.numpy as jnp
from jax import lax
from jax.experimental import pallas as pl
from jax.experimental.pallas import tpu as pltpu
from jax.sharding import PartitionSpec as P

LEARN = 0.05
MESH = pl.DeviceIdType.MESH
LANES = 128
CHUNK = 256
MIB = 1024 * 1024
TILE = 4096
STEP = 16
FINISH = 512
FIRST, SECOND, THIRD, LAST = 4, 8, 14, 24


def parts_of(values):
    high = values.astype(jnp.bfloat16)
    rest = values - high.astype(jnp.float32)
    middle = rest.astype(jnp.bfloat16)
    low = (rest - middle.astype(jnp.float32)).astype(jnp.bfloat16)
    return high, middle, low


def ids_of(info, slots):
    return jnp.concatenate([info[j:j + 1, :] for j in range(info.shape[0])], axis=1)[:, :slots]


def split_into(halves, values):
    count, width = values.shape
    high = values.astype(jnp.bfloat16)
    halves[0:count, 0:width] = high
    halves[0:count, width:2 * width] = (values - high.astype(jnp.float32)).astype(jnp.bfloat16)


def partner(at, step, size):
    if size & (size - 1):
        return lax.rem(at + step, size), lax.rem(at - step + size, size)
    mixed = 0
    bit = 1
    while bit < size:
        mixed = mixed + bit * lax.rem(at // bit + step // bit, 2)
        bit *= 2
    return mixed, mixed


def spread(i, size):
    if size & (size - 1):
        return i
    turned = 0
    bit = 1
    while bit < size:
        turned = turned + (size // (2 * bit)) * lax.rem(i // bit, 2)
        bit *= 2
    return turned


def plan_kernel(slots, rows_dev, code_ref, place, meta, spots):
    devices, lines = meta.shape[0], meta.shape[1]
    deep = lines * LANES
    tall = place.shape[0]
    before = lax.broadcasted_iota(jnp.int32, (CHUNK, CHUNK), 0)
    after = lax.broadcasted_iota(jnp.int32, (CHUNK, CHUNK), 1)
    tri = (before <= after).astype(jnp.bfloat16)
    owners = lax.broadcasted_iota(jnp.int32, (tall, CHUNK), 0)
    lane = lax.broadcasted_iota(jnp.int32, (tall, CHUNK), 1).astype(jnp.float32)
    slot = lax.broadcasted_iota(jnp.int32, (deep, CHUNK), 0)
    base = jnp.full((tall, 1), -1.0, jnp.float32)
    left, right = [], []
    per = CHUNK // LANES
    for b in range(code_ref.shape[0] // per):
        code = jnp.concatenate([code_ref[b * per + j:b * per + j + 1, :] for j in range(per)], axis=1)
        own, at = code // rows_dev, lax.rem(code, rows_dev)
        hit = own == owners
        run = jnp.dot(hit.astype(jnp.bfloat16), tri, preferred_element_type=jnp.float32) + base
        base = run[:, CHUNK - 1:CHUNK]
        spot = jnp.sum(jnp.where(hit, run, 0.0), axis=0, keepdims=True)
        taken = (slot == (spot + 0.5).astype(jnp.int32)).astype(jnp.bfloat16)
        high = (at // LANES + 1).astype(jnp.float32)
        low = lax.rem(at, LANES).astype(jnp.float32)
        fields = jnp.concatenate([
            jnp.where(hit, float(b), 0.0), jnp.where(hit, lane, 0.0),
            jnp.where(hit, high, 0.0), jnp.where(hit, low, 0.0),
        ], axis=0).astype(jnp.bfloat16)
        left.append(fields)
        right.append(taken)
    found = lax.dot_general(
        jnp.concatenate(left, axis=1), jnp.concatenate(right, axis=1),
        (((1,), (1,)), ((), ())), preferred_element_type=jnp.float32)
    whole = (found + 0.5).astype(jnp.int32)
    place[...] = whole[:tall] * CHUNK + whole[tall:2 * tall]
    rows = (whole[2 * tall:3 * tall] - 1) * LANES + whole[3 * tall:]
    for j in range(lines):
        spots[j] = rows[:, j * LANES:(j + 1) * LANES]

    def lay_meta(p, carry):
        for j in range(lines):
            meta[p, j:j + 1, :] = spots[j, pl.ds(p, 1), :]
        return carry

    lax.fori_loop(0, devices, lay_meta, 0, unroll=8 if devices % 8 == 0 else 1)


def kernel(
    n_grp, n_dev, slots, place, meta, grads, hot_grads, hot_slot, hot_ids, table_hbm, acc, block, info,
    gmeta, send, got, halves, part, rbuf, zbuf, total, s_in, s_meta, r_meta, s_big, r_big, s_hot, r_hot,
):
    devices = n_grp * n_dev
    rows_dev, width = acc.shape
    tile = min(TILE, rows_dev)
    lines = meta.shape[1]
    n_lo = n_dev // 2 if n_dev % 2 == 0 else 1
    n_hi = n_dev // n_lo
    plane = n_grp * n_lo
    my_grp, my_dev = lax.axis_index("grp"), lax.axis_index("dev")
    my_hi, my_lo = my_dev // n_lo, lax.rem(my_dev, n_lo)
    me = my_grp * n_dev + my_dev
    seat = my_grp * n_lo + my_lo
    here = (my_grp, my_dev)
    barrier = pltpu.get_barrier_semaphore()

    load = pltpu.make_async_copy(table_hbm, acc, s_in)
    load.start()

    half = n_dev // 2
    own = half * n_grp

    def at_step(k, side):
        a = lax.rem(k, n_grp)
        b = k // n_grp
        b = jnp.where(a == 0, lax.rem(b + n_dev - half, n_dev), b)
        g, d = partner(my_grp, a, n_grp)[side], partner(my_dev, b, n_dev)[side]
        return g * n_dev + d, (g, d)

    def remote(src, dst, ssem, rsem, where):
        return pltpu.make_async_remote_copy(
            src_ref=src, dst_ref=dst, send_sem=ssem, recv_sem=rsem,
            device_id=where, device_id_type=MESH,
        )

    def repeat(first, last, fn):
        def body(k, carry):
            fn(k)
            return carry
        lax.fori_loop(first, last, body, 0)

    def others(first, last, fn):
        def one(k):
            @pl.when(k != own)
            def _():
                fn(k)
        repeat(first, last, one)

    for g in range(n_grp):
        def greet(d, g=g):
            @pl.when(g * n_dev + d != me)
            def _():
                pl.semaphore_signal(barrier, inc=1, device_id=(g, d), device_id_type=MESH)
        repeat(0, n_dev, greet)

    def gather(p, out):
        def body(t, carry):
            first = pl.multiple_of(t * STEP, STEP)
            for j in range(STEP):
                out[p, pl.ds(first + j, 1), :] = grads[pl.ds(place[p, first + j], 1), :]
            return carry
        lax.fori_loop(0, slots // STEP, body, 0)

    def pack(k):
        gather(at_step(k, 0)[0], send)

    def launch(k):
        p, where = at_step(k, 0)
        remote(send.at[p], got.at[me], s_big, r_big.at[k], where).start()

    def pack_then_launch(k):
        pack(k)

        @pl.when(k - 1 != own)
        def _():
            launch(k - 1)

    def send_meta(k):
        p, where = at_step(k, 0)
        remote(meta.at[p], gmeta.at[me], s_meta, r_meta, where).start()

    def across(buf_from, at_from, buf_to, at_to, sems):
        def one(j):
            g, lo = partner(my_grp, j // n_lo, n_grp)[0], partner(my_lo, lax.rem(j, n_lo), n_lo)[0]
            src = at_from(g * n_lo + lo)
            remote(buf_from.at[src], buf_to.at[at_to], s_hot.at[sems], r_hot.at[sems], (g, my_hi * n_lo + lo)).start()
        repeat(1, plane, one)

    def finish(buf, count, sems):
        if count:
            most = pl.ds(0, count)
            done = remote(buf.at[most], buf.at[most], s_hot.at[sems], r_hot.at[sems], here)
            done.wait_recv()
            done.wait_send()

    def up(j):
        hi = partner(my_hi, j, n_hi)[0]
        remote(zbuf.at[my_hi], zbuf.at[my_hi], s_hot.at[1], r_hot.at[1], (my_grp, hi * n_lo + my_lo)).start()

    pack(0)
    pack(1)
    pl.semaphore_wait(barrier, devices - 1)
    launch(0)
    repeat(2, FIRST, pack_then_launch)
    others(0, devices, send_meta)
    hot = plane * part.shape[1]
    pick = lax.broadcasted_iota(jnp.int32, (hot, hot_grads.shape[0]), 0) == hot_slot[...]
    split = jnp.concatenate(parts_of(hot_grads[...]), axis=1)
    three = jnp.dot(pick.astype(jnp.bfloat16), split, preferred_element_type=jnp.float32)
    part[...] = (three[:, :width] + three[:, width:2 * width] + three[:, 2 * width:]).reshape(part.shape)
    gmeta[me] = meta[me]
    rbuf[seat] = part[seat]
    cuts = [FIRST, FIRST + 1, SECOND, SECOND + 1, THIRD, THIRD + 1, devices]
    repeat(cuts[0], cuts[1], pack_then_launch)
    across(part, lambda other: other, rbuf, seat, 0)
    repeat(cuts[1], cuts[2], pack_then_launch)
    finish(rbuf, plane - 1, 0)
    zbuf[my_hi] = jnp.sum(rbuf[...], axis=0)
    repeat(cuts[2], cuts[3], pack_then_launch)
    repeat(1, n_hi, up)
    repeat(cuts[3], cuts[4], pack_then_launch)
    finish(zbuf, n_hi - 1, 1)
    total[seat] = jnp.sum(zbuf[...], axis=0)
    repeat(cuts[4], cuts[5], pack_then_launch)
    across(total, lambda other: seat, total, seat, 2)
    repeat(cuts[5], cuts[6], pack_then_launch)
    gather(me, got)
    others(devices - 1, devices, launch)
    load.wait()

    metas = remote(meta.at[pl.ds(0, devices - 1)], gmeta.at[pl.ds(0, devices - 1)], s_meta, r_meta, here)

    def add(values, ids):
        count = values.shape[0]
        split_into(halves, values)
        spot = lax.broadcasted_iota(jnp.int32, (tile, count), 0)

        def body(t, carry):
            at = pl.multiple_of(t * tile, tile)
            hit = jnp.where(spot == ids - at, 1.0, 0.0).astype(jnp.bfloat16)
            both = jnp.dot(hit, halves[0:count, :], preferred_element_type=jnp.float32)
            w = pl.ds(at, tile)
            acc[w, :] = acc[w, :] - LEARN * (both[:, :width] + both[:, width:])
            return carry

        lax.fori_loop(0, rows_dev // tile, body, 0)

    metas.wait_send()
    metas.wait_recv()

    def turn(k):
        @pl.when(k == LAST)
        def _():
            finish(total, plane - 1, 2)
            count = hot_ids.shape[1]
            add(total[...].reshape(-1, width)[:count], hot_ids[...] - me * rows_dev)

        source = at_step(k, 1)[0]

        @pl.when(k != own)
        def _():
            remote(send.at[0], got.at[source], s_big, r_big.at[k], here).wait_recv()

        @pl.when(k < devices - 1)
        def _():
            add(got[source], ids_of(gmeta[source], slots))

        @pl.when(k == devices - 1)
        def _():
            block[...] = got[source]
            info[...] = gmeta[source]

    repeat(0, devices, turn)
    most = pl.ds(0, devices - 1)
    remote(send.at[most], got.at[most], s_big, r_big.at[0], here).wait_send()


def finish_kernel(slots, acc, block, info, out, ready, halves, sems):
    rows_dev, width = acc.shape
    tile = min(FINISH, rows_dev)
    ids = ids_of(info[...], slots)
    split_into(halves, block[...])
    spot = lax.broadcasted_iota(jnp.int32, (tile, slots), 0)
    copies = []
    for t in range(rows_dev // tile):
        w = pl.ds(t * tile, tile)
        hit = jnp.where(spot == ids - t * tile, 1.0, 0.0).astype(jnp.bfloat16)
        both = jnp.dot(hit, halves[...], preferred_element_type=jnp.float32)
        ready[w, :] = acc[w, :] - LEARN * (both[:, :width] + both[:, width:])
        copies.append(pltpu.make_async_copy(ready.at[w], out.at[w], sems.at[t]))
        copies[-1].start()
    for copy in copies:
        copy.wait()


def on_device(n_grp, n_dev, table, cold_grads, cold_owner, cold_row, hot_grads, hot_slot, hot_ids):
    devices = n_grp * n_dev
    rows_dev, width = table.shape
    lookups = cold_grads.shape[0]
    looks = hot_grads.shape[0]
    hot = hot_ids.shape[0]
    slots = -(-2 * lookups // devices // STEP) * STEP
    tall = -(-devices // 8) * 8
    lines = -(-slots // LANES)
    n_lo = n_dev // 2 if n_dev % 2 == 0 else 1
    plane = n_grp * n_lo
    share = -(-hot // (plane * 8)) * 8
    vmem, hbm = pl.BlockSpec(memory_space=pltpu.VMEM), pl.BlockSpec(memory_space=pltpu.HBM)
    f32, i32 = jnp.float32, jnp.int32
    dma = pltpu.SemaphoreType.DMA
    smem = pl.BlockSpec(memory_space=pltpu.SMEM)
    place, meta = pl.pallas_call(
        functools.partial(plan_kernel, slots, rows_dev),
        out_shape=(
            jax.ShapeDtypeStruct((tall, lines * LANES), i32),
            jax.ShapeDtypeStruct((devices, lines, LANES), i32),
        ),
        in_specs=[vmem],
        out_specs=(vmem,) * 2,
        scratch_shapes=[pltpu.VMEM((lines, tall, LANES), i32)],
        compiler_params=pltpu.CompilerParams(vmem_limit_bytes=8 * MIB),
        cost_estimate=pl.CostEstimate(flops=10 ** 11, bytes_accessed=MIB, transcendentals=0),
        name="plan",
    )((cold_owner * rows_dev + cold_row.reshape(-1, 1)).reshape(-1, LANES))
    blocks = (devices, slots, width)
    shares = (plane, share, width)
    acc, block, info = pl.pallas_call(
        functools.partial(kernel, n_grp, n_dev, slots),
        out_shape=(
            jax.ShapeDtypeStruct(table.shape, f32),
            jax.ShapeDtypeStruct(blocks[1:], f32),
            jax.ShapeDtypeStruct((lines, LANES), i32),
        ),
        in_specs=[smem, vmem, vmem, vmem, vmem, vmem, hbm],
        out_specs=(vmem,) * 3,
        scratch_shapes=[
            pltpu.VMEM((devices, lines, LANES), i32),
            pltpu.VMEM(blocks, f32),
            pltpu.VMEM(blocks, f32),
            pltpu.VMEM((max(slots, hot), 2 * width), jnp.bfloat16),
            pltpu.VMEM(shares, f32),
            pltpu.VMEM(shares, f32),
            pltpu.VMEM((n_dev // n_lo, share, width), f32),
            pltpu.VMEM(shares, f32),
            dma, dma, dma, dma, dma((devices,)), dma((3,)), dma((3,)),
        ],
        compiler_params=pltpu.CompilerParams(
            collective_id=0, has_side_effects=True, vmem_limit_bytes=44 * MIB
        ),
        name="update",
    )(place, meta, cold_grads, hot_grads, hot_slot.reshape(1, -1), hot_ids.reshape(1, -1), table)
    return pl.pallas_call(
        functools.partial(finish_kernel, slots),
        out_shape=jax.ShapeDtypeStruct(table.shape, f32),
        in_specs=[vmem] * 3,
        out_specs=hbm,
        scratch_shapes=[
            pltpu.VMEM(table.shape, f32),
            pltpu.VMEM((slots, 2 * width), jnp.bfloat16),
            dma((-(-rows_dev // FINISH),)),
        ],
        compiler_params=pltpu.CompilerParams(vmem_limit_bytes=24 * MIB),
        name="finish",
    )(acc, block, info)


def solution(mesh):
    in_specs = (
        P(("grp", "dev"), None),
        P(("grp", "dev"), None),
        P(("grp", "dev"), None),
        P(("grp", "dev")),
        P(("grp", "dev"), None),
        P(("grp", "dev")),
        P(),
    )
    out_specs = P(("grp", "dev"), None)
    return jax.shard_map(
        functools.partial(on_device, mesh.shape["grp"], mesh.shape["dev"]),
        mesh=mesh, in_specs=in_specs, out_specs=out_specs, check_vma=False,
    )
```
